256 devices in a mesh: expert: 64 (over x, z, core), rep: 4 (over y).
Axes of the slice: x: 4, y: 4, z: 8, core: 2. Of those that a mesh axis runs over, the one named last changes fastest.
Arguments:
- features: bfloat16 [32768, 1024], P(('expert', 'rep')), may hold values from -20 to 20
- readout: bfloat16 [32768, 1024], P(('expert', 'rep')), may hold values from -20 to 20
- up_weight: bfloat16 [64, 1024, 2048], P('expert'), may hold values from -0.1875 to 0.1875
- down_weight: bfloat16 [64, 2048, 1024], P('expert'), may hold values from -0.125 to 0.125
- expert_ids: int32 [32768, 2], P(('expert', 'rep')), may hold values from 0 to 63, all different within a row; in each aligned block of 128 rows (0 to 127, 128 to 255, ...) at most 5 rows name the same one
- gate_values: float32 [32768, 2], P(('expert', 'rep')), may hold values from 0.2 to 1
Outputs:
- grad_up: bfloat16 [64, 1024, 2048], P('expert', 'rep')
- input_grad: float32 [32768, 1024], P(('expert', 'rep'))
- penalty: float32 [], replicated
The draws below stay inside these ranges and needn't reach their ends.
Inputs may be any that keep to these rules, and one draw needn't show every extreme that they name: `expert_ids`: each row names 2 different experts. In each aligned block of 128 rows (the rows of one device) no expert is named more than 5 times, a bound that some block reaches.
All inputs are finite; a program needn't handle non-finite values.
Results may differ from the reference program's by a relative error of at most 0.01.
Values may be sent and summed in bfloat16 or wider, within the bound.
A program may use at most 128 MiB of HBM per device.

```python
import math
import jax
import jax.numpy as jnp
import numpy as np
from jax import lax

D = 1024
FF = 2048
TOPK = 2
TOK_DEV = 128
EXPERTS = 64
TOKENS = 32768
CAP = 5
N_EXPERT = 64
N_REP = 4


def draw_features(key, part):
    key_base, key_scale = jax.random.split(jax.random.fold_in(key, 11), 2)
    rising = 3.0 ** (jnp.arange(TOKENS, dtype=jnp.float32) / (TOKENS - 1))
    baseline = jax.random.normal(key_base, (TOKENS, D), jnp.float32)
    row_scale = jax.random.uniform(key_scale, (TOKENS, 1), jnp.float32, 0.7, 1.3)
    return jnp.clip(baseline * row_scale * rising[:, None], -20.0, 20.0).astype(jnp.bfloat16)


def draw_readout(key, part):
    key_base, key_scale = jax.random.split(jax.random.fold_in(key, 23), 2)
    rising = 3.0 ** (jnp.arange(TOKENS, dtype=jnp.float32) / (TOKENS - 1))
    baseline = jax.random.normal(key_base, (TOKENS, D), jnp.float32)
    row_scale = jax.random.uniform(key_scale, (TOKENS, 1), jnp.float32, 0.7, 1.3)
    return jnp.clip(baseline * row_scale * rising[:, None], -20.0, 20.0).astype(jnp.bfloat16)


def block_levels(rng, shape, pieces, low, high):
    level = 1.0
    for dim, parts in pieces:
        heights = jax.random.uniform(jax.random.fold_in(jax.random.fold_in(rng, 6), dim), (parts,), jnp.float32, low / len(pieces), high / len(pieces))
        level = level * jnp.repeat(jnp.exp(heights), shape[dim] // parts).reshape((-1,) + (1,) * (len(shape) - 1 - dim))
    return level


def shared_out(stream_key, own, number, rows, amount, top, most, slope):
    sequence = jax.random.permutation(stream_key, amount)
    packed, ordinary = portions_of(amount, rows * top, most, slope, True), portions_of(amount, rows * top, most, slope, False)
    places = jnp.arange(amount)

    def named(tallies, offset_by):
        used = int((tallies > 0).sum())
        fixed = max(1, used // 4)
        passed = fixed + (places - fixed + offset_by * (used - fixed)) % max(1, amount - fixed)
        return jnp.zeros((amount,), jnp.int32).at[sequence[jnp.where(places < fixed, places, passed)]].set(jnp.asarray(tallies, jnp.int32))

    tallies = jnp.where(number % 4 == 0, named(packed, number // 4), named(ordinary, number - number // 4 - 1))
    mixed = jax.random.permutation(jax.random.fold_in(own, 3), amount)
    donor, sink = mixed[0:amount // 2 * 2:2], mixed[1:amount // 2 * 2:2]
    margin = jnp.minimum(tallies[donor] - 1, most - tallies[sink]) // 2
    margin = jnp.where((donor == sequence[0]) | (sink == sequence[0]) | (tallies[sink] == 0), 0, jnp.maximum(margin, 0))
    passed = jax.random.randint(jax.random.fold_in(own, 4), (amount // 2,), 0, 1 << 20) % (margin + 1)
    tallies = tallies.at[donor].add(-passed).at[sink].add(passed)
    labels = jnp.searchsorted(jnp.cumsum(tallies), jnp.arange(rows * top), side="right").astype(jnp.int32)
    table = labels.reshape(top, rows).T
    table = table[jax.random.permutation(jax.random.fold_in(own, 1), rows)]
    offset_by = jax.random.randint(jax.random.fold_in(own, 2), (rows, 1), 0, top)
    return jnp.take_along_axis(table, (jnp.arange(top)[None, :] + offset_by) % top, axis=1)


def portions_of(amount, total, limit, skew, full):
    portions = [(1 << 20) // math.isqrt(grade ** skew) + 1 for grade in range(1, amount + 1)]
    largest = limit if full else min(limit, max(-(-total // amount), total * portions[0] // sum(portions)))
    least = 1 if total - largest >= amount - 1 else 0
    counts, rest = [largest] + [least] * (amount - 1), total - largest - least * (amount - 1)
    while rest > 0:
        candidates = [i for i in range(1, amount) if counts[i] < largest] or [i for i in range(1, amount) if counts[i] < limit]
        mass, left = sum([portions[i] for i in candidates]), rest
        for i in candidates:
            extra = min(limit - counts[i], max(1, left * portions[i] // mass), rest)
            counts[i] = counts[i] + extra
            rest = rest - extra
    return np.array(counts)


def gaussian(stream_key, extent, width, most, shards=(), kind=jnp.bfloat16):
    drawn = width * jax.random.normal(stream_key, extent, jnp.float32)
    if shards:
        drawn = drawn * block_levels(stream_key, extent, shards, -0.22, 0.18)
    return jnp.clip(drawn, -most, most).astype(kind)


def setup_inputs(seed: int = 0) -> dict:
    key_of = jax.random.split(jax.random.key(seed), 7)
    features = draw_features(jax.random.fold_in(key_of[6], 71), 0)
    readout = draw_readout(jax.random.fold_in(key_of[6], 71), 0)
    up_weight = gaussian(key_of[2], (EXPERTS, D, FF), D ** -0.5, 0.1875, ((0, 64),))
    down_weight = gaussian(key_of[3], (EXPERTS, FF, D), FF ** -0.5, 0.125, ((0, 64),))
    expert_ids_keys = jax.random.split(jax.random.fold_in(key_of[4], 1), TOKENS // TOK_DEV)
    expert_ids_turns = jax.random.permutation(jax.random.fold_in(key_of[4], 3), TOKENS // TOK_DEV)
    expert_ids = jax.vmap(lambda own, number: shared_out(jax.random.fold_in(key_of[4], 2), own, number, TOK_DEV, EXPERTS, TOPK, CAP, 1))(expert_ids_keys, expert_ids_turns).reshape((TOKENS, TOPK))
    gate_values = jnp.clip(0.2 + 0.8 * jax.random.uniform(key_of[5], (TOKENS, TOPK), jnp.float32) ** block_levels(key_of[5], (TOKENS, TOPK), ((0, 256),), -0.2, 0.2), 0.2, 1.0)
    return {"features": features, "readout": readout, "up_weight": up_weight, "down_weight": down_weight, "expert_ids": expert_ids, "gate_values": gate_values}


def silu_slopes(pre_act):
    logistic = jax.nn.sigmoid(pre_act)
    first = logistic * (1.0 + pre_act * (1.0 - logistic))
    second = logistic * (1.0 - logistic) * (2.0 + pre_act * (1.0 - 2.0 * logistic))
    return first, second


def contract_last(left, right):
    return lax.dot_general(left, right, (((1,), (1,)), ((), ())), preferred_element_type=jnp.float32)


def expert_hidden(slot_x, slot_r, up_matrix, down_matrix):
    pre_act = jnp.dot(slot_x, up_matrix, preferred_element_type=jnp.float32)
    projected = jnp.dot(slot_r, down_matrix.T, preferred_element_type=jnp.float32)
    first, second = silu_slopes(pre_act)
    scaled = (first * projected).astype(jnp.bfloat16)
    return scaled, pre_act, projected


def by_copy(values):
    cols = values.shape[1]
    shaped = values.reshape(N_EXPERT, N_REP, CAP, cols).transpose(1, 0, 2, 3)
    return shaped.reshape(N_REP, N_EXPERT * CAP, cols).astype(jnp.float32)


def reference(features, readout, up_weight, down_weight, expert_ids, gate_values):
    tokens_all = features.shape[0]
    blocks = tokens_all // TOK_DEV
    block_ids = expert_ids.reshape(blocks, 2 * TOK_DEV)
    onehot = (block_ids[:, :, None] == jnp.arange(EXPERTS, dtype=jnp.int32)[None, None, :]).astype(jnp.int32)
    earlier = jnp.cumsum(onehot, axis=1) - onehot
    slot_index = jnp.sum(earlier * onehot, axis=2).astype(jnp.int32)
    position = (jnp.arange(blocks, dtype=jnp.int32)[:, None] * CAP + slot_index).reshape(-1).astype(jnp.int32)
    flat_ids = expert_ids.reshape(-1).astype(jnp.int32)
    pair_count = 2 * tokens_all
    table = jnp.full((EXPERTS, blocks * CAP), pair_count, jnp.int32)
    table = table.at[flat_ids, position].set(jnp.arange(pair_count, dtype=jnp.int32))
    zero_row = jnp.zeros((1, D), jnp.bfloat16)
    padded_x = jnp.concatenate([features, zero_row], axis=0)
    padded_r = jnp.concatenate([readout, zero_row], axis=0)

    def gather_slots(table_row):
        token_index = (table_row // 2).astype(jnp.int32)
        return padded_x[token_index], padded_r[token_index]

    def forward(operands):
        up_matrix, down_matrix, table_row = operands
        slot_x, slot_r = gather_slots(table_row)
        scaled, pre_act, projected = expert_hidden(slot_x, slot_r, up_matrix, down_matrix)
        return contract_last(scaled, up_matrix).astype(jnp.bfloat16)

    outputs = lax.map(forward, (up_weight, down_weight, table))
    pair_out = outputs[flat_ids, position].astype(jnp.float32).reshape(tokens_all, 2, D)
    input_grad = readout.astype(jnp.float32) + gate_values[:, 0:1] * pair_out[:, 0] + gate_values[:, 1:2] * pair_out[:, 1]
    penalty = jnp.sum(input_grad * input_grad) / (2.0 * tokens_all * D)
    cotangent = (gate_values[:, :, None] * input_grad[:, None, :]).reshape(pair_count, D).astype(jnp.bfloat16)
    padded_w = jnp.concatenate([cotangent, zero_row], axis=0)

    def backward(operands):
        up_matrix, down_matrix, table_row = operands
        slot_x, slot_r = gather_slots(table_row)
        slot_w = padded_w[table_row]
        scaled, pre_act, projected = expert_hidden(slot_x, slot_r, up_matrix, down_matrix)
        first, second = silu_slopes(pre_act)
        slope_grad = jnp.dot(slot_w, up_matrix, preferred_element_type=jnp.float32)
        pre_grad = (slope_grad * projected * second).astype(jnp.bfloat16)
        term = jnp.einsum("rsd,rsf->rdf", by_copy(slot_w), by_copy(scaled))
        term = term + jnp.einsum("rsd,rsf->rdf", by_copy(slot_x), by_copy(pre_grad))
        rounded = lax.optimization_barrier(term.astype(jnp.bfloat16)).astype(jnp.float32)
        return jnp.sum(rounded, axis=0).astype(jnp.bfloat16)

    grad_up = lax.map(backward, (up_weight, down_weight, table))
    return grad_up, input_grad, penalty
```

```python
import functools

import jax
import jax.numpy as jnp
import numpy as np
from jax import lax
from jax.experimental import pallas as pl
from jax.experimental.pallas import tpu as pltpu
from jax.sharding import PartitionSpec as P

MESH = pl.DeviceIdType.MESH
F32 = jnp.float32
BF16 = jnp.bfloat16
NX, NZ, NC, CAP = 4, 8, 2, 5


def dot(a, b):
    return lax.dot_general(a, b, (((1,), (0,)), ((), ())), preferred_element_type=F32)


def dot_t(a, b):
    return lax.dot_general(a, b, (((1,), (1,)), ((), ())), preferred_element_type=F32)


def kernel(
    dims,
    x_ref, r_ref, up_hbm, down_hbm, ids_ref, gate_ref, pf_ref, pb_ref,
    grad_ref, ig_ref, pen_ref,
    up, down, sz, rz, sx, rx, ax, ar, slope, curve, proj, sg, scaled, pgrad, xt, wt,
    sel, selt, rs_s, rs_r, q_r, q_g, q_y,
    wsem, zs, zr, xs, xr, rss, rsr, qs, qr,
):
    nx, nz, nc, ny, cap = dims
    ng = nx * nc
    tok, width = x_ref.shape
    ff = up.shape[1]
    half = width // 2
    zrow, grow = ng * cap, nz * cap
    slots = nz * zrow
    e = lax.axis_index("expert")
    y = lax.axis_index("rep")
    x = e // (nz * nc)
    z = (e // nc) % nz
    c = e % nc
    g = x * nc + c

    def z_peer(k):
        zt = lax.rem(z + k, nz)
        return zt, ((x * nz + zt) * nc + c, y)

    def g_peer(k):
        gt = lax.rem(g + k, ng)
        return gt, (((gt // nc) * nz + z) * nc + gt % nc, y)

    def y_peer(k):
        yt = lax.rem(y + k, ny)
        return yt, (e, yt)

    load_up = pltpu.make_async_copy(up_hbm.at[0], up, wsem.at[0])
    load_down = pltpu.make_async_copy(down_hbm.at[0], down, wsem.at[1])
    load_up.start()
    load_down.start()

    barrier = pltpu.get_barrier_semaphore()
    peers = (
        [z_peer(k)[1] for k in range(1, nz)]
        + [g_peer(k)[1] for k in range(1, ng)]
        + [y_peer(k)[1] for k in range(1, ny)]
    )
    for peer in peers:
        pl.semaphore_signal(barrier, inc=1, device_id=peer, device_id_type=MESH)

    zorder = sorted(range(1, nz), key=lambda k: (-min(k, nz - k), k))
    gorder = sorted(range(1, ng), key=lambda k: (-min(k, ng - k), k))

    def z_send(st):
        for k in zorder:
            zt, dev = z_peer(k)
            pltpu.make_async_remote_copy(
                src_ref=sz.at[st, zt], dst_ref=rz.at[st, z],
                send_sem=zs.at[st], recv_sem=zr.at[st],
                device_id=dev, device_id_type=MESH,
            ).start()

    def g_send(st):
        for k in gorder:
            gt, dev = g_peer(k)
            pltpu.make_async_remote_copy(
                src_ref=sx.at[st, gt], dst_ref=rx.at[st, g],
                send_sem=xs.at[st], recv_sem=xr.at[st],
                device_id=dev, device_id_type=MESH,
            ).start()

    def wait_all(ref, st, count, sem):
        part = ref.at[st, pl.ds(0, count)]
        pltpu.make_async_copy(part, part, sem.at[st]).wait()

    def z_wait(st):
        wait_all(rz, st, nz - 1, zr)
        rz[st, z] = sz[st, z]

    def g_wait(st):
        wait_all(rx, st, ng - 1, xr)
        rx[st, g] = sx[st, g]

    def flat(ref, st):
        v = ref[st].astype(F32)
        return v.reshape(slots, half).astype(BF16)

    def put(ref, st, v):
        shape = ref.shape[1:]
        ref[st] = v.reshape(shape).astype(BF16)

    n_exp = nz * ng
    col_e = lax.broadcasted_iota(jnp.int32, (tok, n_exp), 1)
    onehots = []
    orders = []
    for k in range(2):
        v = ids_ref[:, k : k + 1]
        rest = v // nc if nc > 1 else v
        q = (rest % nz) * ng + (rest // nz) * nc + (v % nc if nc > 1 else 0)
        orders.append(q)
        onehots.append(jnp.where(col_e == q, 1.0, 0.0).astype(F32))
    count = (onehots[0] + onehots[1]).astype(BF16)
    ti = lax.broadcasted_iota(jnp.int32, (tok, tok), 0)
    tj = lax.broadcasted_iota(jnp.int32, (tok, tok), 1)
    lower = jnp.where(tj < ti, 1.0, 0.0).astype(BF16)
    earlier = dot(lower, count)
    col_s = lax.broadcasted_iota(jnp.int32, (tok, slots), 1).astype(F32)
    for k in range(2):
        slot = jnp.sum(onehots[k] * earlier, axis=1, keepdims=True)
        pos = orders[k].astype(F32) * cap + slot
        m = jnp.where(col_s == pos, 1.0, 0.0).astype(F32)
        sel[k] = m.astype(BF16)
        selt[k] = m.T.astype(BF16)

    both = (selt[0].astype(F32) + selt[1].astype(F32)).astype(BF16)
    for h in range(2):
        put(sz, h, dot(both, x_ref[:, h * half : (h + 1) * half]))
    pl.semaphore_wait(barrier, len(peers))
    z_send(0)
    z_send(1)
    for h in range(2):
        put(sz, 2 + h, dot(both, r_ref[:, h * half : (h + 1) * half]))
        z_send(2 + h)

    def forward(st):
        z_wait(st)
        put(sx, st, dot(pf_ref[...], flat(rz, st)))
        g_send(st)

    tile = 256
    forward(0)
    forward(1)
    load_up.wait()
    load_down.wait()
    for h in range(2):
        g_wait(h)
        ax[:, h * half : (h + 1) * half] = flat(rx, h)

    @pl.loop(0, ff // tile)
    def _(i):
        n = pl.ds(pl.multiple_of(i * tile, tile), tile)
        p = dot(ax[...], up[:, n])
        s = 1.0 / (1.0 + jnp.exp(-p))
        slope[:, n] = s * (1.0 + p * (1.0 - s))
        curve[:, n] = s * (1.0 - s) * (2.0 + p * (1.0 - 2.0 * s))

    forward(2)
    forward(3)
    g_wait(2)
    ar[:, :half] = flat(rx, 2)

    @pl.loop(0, ff // tile)
    def _(i):
        n = pl.ds(pl.multiple_of(i * tile, tile), tile)
        proj[:, n] = dot_t(ar[:, :half], down[n, :half])

    g_wait(3)
    ar[:, half:] = flat(rx, 3)

    @pl.loop(0, ff // tile)
    def _(i):
        n = pl.ds(pl.multiple_of(i * tile, tile), tile)
        p = proj[:, n] + dot_t(ar[:, half:], down[n, half:])
        scaled[:, n] = (slope[:, n] * p).astype(BF16)
        proj[:, n] = p * curve[:, n]

    for h in range(2):
        for i in range(half // tile if half > tile else 1):
            w = min(tile, half)
            lo = i * w
            v = dot_t(scaled[...], up[h * half + lo : h * half + lo + w, :])
            sx[4 + h, :, :, lo : lo + w] = v.reshape(ng, grow, w).astype(BF16)
        g_send(4 + h)
    for h in range(2):
        g_wait(4 + h)
        put(sz, 4 + h, dot(pb_ref[...], flat(rx, 4 + h)))
        z_send(4 + h)

    xt[...] = ax[...].astype(F32).T.astype(BF16)

    squares = jnp.zeros((8, 128), F32)
    for h in range(2):
        cols = slice(h * half, (h + 1) * half)
        z_wait(4 + h)
        got = flat(rz, 4 + h)
        g0 = gate_ref[:, 0:1]
        g1 = gate_ref[:, 1:2]
        ig = r_ref[:, cols].astype(F32) + g0 * dot(sel[0], got) + g1 * dot(sel[1], got)
        ig_ref[:, cols] = ig
        cot = dot(selt[0], (g0 * ig).astype(BF16)) + dot(selt[1], (g1 * ig).astype(BF16))
        put(sz, 6 + h, cot)
        z_send(6 + h)
        sq = (ig * ig).reshape(tok // 8, 8, half // 128, 128)
        squares = squares + jnp.sum(jnp.sum(sq, axis=0), axis=1)

    def q_send(buf, me, peer_of, n, st):
        for k in range(1, n):
            _, dev = peer_of(k)
            pltpu.make_async_remote_copy(
                src_ref=buf.at[me], dst_ref=buf.at[me],
                send_sem=qs.at[st], recv_sem=qr.at[st],
                device_id=dev, device_id_type=MESH,
            ).start()

    def q_wait(buf, n, st):
        part = buf.at[pl.ds(0, n - 1)]
        pltpu.make_async_copy(part, part, qr.at[st]).wait()
        pltpu.make_async_copy(part, part, qs.at[st]).wait()
        total = buf[0]
        for i in range(1, n):
            total = total + buf[i]
        return total

    q_r[z] = squares
    q_send(q_r, z, z_peer, nz, 0)

    for st in (6, 7):
        forward(st)
    q_g[g] = q_wait(q_r, nz, 0)
    q_send(q_g, g, g_peer, ng, 1)

    g_wait(6)
    first = flat(rx, 6)
    wt[:half] = first.astype(F32).T.astype(BF16)

    @pl.loop(0, ff // tile)
    def _(i):
        n = pl.ds(pl.multiple_of(i * tile, tile), tile)
        sg[:, n] = dot(flat(rx, 6), up[:half, n])

    g_wait(7)
    wt[half:] = flat(rx, 7).astype(F32).T.astype(BF16)

    @pl.loop(0, ff // tile)
    def _(i):
        n = pl.ds(pl.multiple_of(i * tile, tile), tile)
        s = sg[:, n] + dot(flat(rx, 7), up[half:, n])
        pgrad[:, n] = (s * proj[:, n]).astype(BF16)

    q_y[y] = q_wait(q_g, ng, 1)
    q_send(q_y, y, y_peer, ny, 2)

    rows = width // ny
    parts = rs_s.shape[2]
    piece = ff // 2 // parts

    def unit(block, d, j):
        rb = pl.ds(pl.multiple_of(block * rows, rows), rows)
        cb = pl.ds(pl.multiple_of(d * (ff // 2) + j * piece, piece), piece)
        v = dot(wt[rb, :], scaled[:, cb]) + dot(xt[rb, :], pgrad[:, cb])
        return v.astype(BF16).astype(F32), cb

    def rs_copy(t, d, j):
        _, dev = y_peer(1 if d == 0 else ny - 1)
        return pltpu.make_async_remote_copy(
            src_ref=rs_s.at[d, t, j], dst_ref=rs_r.at[d, t, j],
            send_sem=rss.at[d, t, j], recv_sem=rsr.at[d, t, j],
            device_id=dev, device_id_type=MESH,
        )

    for t in range(ny):
        @pl.loop(0, parts)
        def _(j):
            for d in range(2):
                step = t + 1
                block = lax.rem(y + (ny - step if d == 0 else step), ny)
                v, cb = unit(block, d, j)
                if t > 0:
                    rs_copy(t - 1, d, j).wait_recv()
                    v = v + rs_r[d, t - 1, j].astype(F32)
                if t < ny - 1:
                    rs_s[d, t, j] = v.astype(BF16)
                    rs_copy(t, d, j).start()
                else:
                    grad_ref[0, :, cb] = v.astype(BF16)

    total = q_wait(q_y, ny, 2)
    total = jnp.sum(jnp.sum(total, axis=0, keepdims=True), axis=1, keepdims=True)
    pen_ref[...] = jnp.broadcast_to(total, pen_ref.shape)

    @pl.loop(0, parts)
    def _(j):
        for t in range(ny - 1):
            for d in range(2):
                rs_copy(t, d, j).wait_send()

    for st in range(8):
        wait_all(sz, st, nz - 1, zs)
        wait_all(sx, st, ng - 1, xs)


def regroup(outer, inner, cap):
    n = outer * inner * cap
    src = np.arange(n).reshape(outer, inner, cap).transpose(1, 0, 2).reshape(-1)
    return jnp.asarray(np.eye(n, dtype=np.float32)[src], BF16)


def body(dims, features, readout, up_weight, down_weight, expert_ids, gate_values):
    nx, nz, nc, ny, cap = dims
    ng = nx * nc
    tok, width = features.shape
    ff = up_weight.shape[2]
    half = width // 2
    slots = nz * ng * cap
    parts = max(1, ff // 2 // 256)
    vm = pl.BlockSpec(memory_space=pltpu.VMEM)
    hbm = pl.BlockSpec(memory_space=pl.ANY)
    dma = pltpu.SemaphoreType.DMA
    zbuf = pltpu.VMEM((8, nz, ng * cap, half), BF16)
    gbuf = pltpu.VMEM((8, ng, nz * cap, half), BF16)
    wide = pltpu.VMEM((slots, ff), F32)
    ring = pltpu.VMEM((2, ny - 1, parts, width // ny, ff // 2 // parts), BF16)
    grad, ig, pen = pl.pallas_call(
        functools.partial(kernel, dims),
        out_shape=(
            jax.ShapeDtypeStruct((1, width // ny, ff), BF16),
            jax.ShapeDtypeStruct((tok, width), F32),
            jax.ShapeDtypeStruct((8, 128), F32),
        ),
        in_specs=[vm, vm, hbm, hbm, vm, vm, vm, vm],
        out_specs=(vm, vm, vm),
        scratch_shapes=[
            pltpu.VMEM((width, ff), BF16),
            pltpu.VMEM((ff, width), BF16),
            zbuf, zbuf, gbuf, gbuf,
            pltpu.VMEM((slots, width), BF16),
            pltpu.VMEM((slots, width), BF16),
            wide, wide, wide, wide,
            pltpu.VMEM((slots, ff), BF16),
            pltpu.VMEM((slots, ff), BF16),
            pltpu.VMEM((width, slots), BF16),
            pltpu.VMEM((width, slots), BF16),
            pltpu.VMEM((2, tok, slots), BF16),
            pltpu.VMEM((2, slots, tok), BF16),
            ring, ring,
            pltpu.VMEM((nz, 8, 128), F32),
            pltpu.VMEM((ng, 8, 128), F32),
            pltpu.VMEM((ny, 8, 128), F32),
            dma((2,)), dma((8,)), dma((8,)), dma((8,)), dma((8,)),
            dma((2, ny - 1, parts)), dma((2, ny - 1, parts)),
            dma((3,)), dma((3,)),
        ],
        compiler_params=pltpu.CompilerParams(
            collective_id=0, has_side_effects=True, vmem_limit_bytes=67043328
        ),
    )(
        features, readout, up_weight, down_weight, expert_ids, gate_values,
        regroup(nz, ng, cap), regroup(ng, nz, cap),
    )
    groups = nz * ng
    penalty = pen[0, 0] / (2.0 * tok * groups * ny * width)
    return grad, ig, penalty


def solution(mesh, dims=None):
    if dims is None:
        dims = (NX, NZ, NC, mesh.shape["rep"], CAP)
    both = ("expert", "rep")
    return jax.shard_map(
        functools.partial(body, dims),
        mesh=mesh,
        in_specs=(
            P(both, None), P(both, None),
            P("expert", None, None), P("expert", None, None),
            P(both, None), P(both, None),
        ),
        out_specs=(P("expert", "rep", None), P(both, None), P()),
        check_vma=False,
    )
```

```python
import functools

import jax
import jax.numpy as jnp
import numpy as np
from jax import lax
from jax.experimental import pallas as pl
from jax.experimental.pallas import tpu as pltpu
from jax.sharding import PartitionSpec as P

MESH = pl.DeviceIdType.MESH
F32 = jnp.float32
BF16 = jnp.bfloat16
NX, NZ, NC, CAP = 4, 8, 2, 5
TILE = 256


def dot(a, b):
    return lax.dot_general(a, b, (((1,), (0,)), ((), ())), preferred_element_type=F32)


def dot_t(a, b):
    return lax.dot_general(a, b, (((1,), (1,)), ((), ())), preferred_element_type=F32)


def kernel(
    dims,
    x_ref, r_ref, up_hbm, down_hbm, ids_ref, gate_ref, pf_ref, pb_ref,
    grad_ref, ig_ref, pen_ref,
    up, down, sz, rz, sx, rx, ry, act, sg, pc, scaled, xt, wt, gacc,
    sel, selt, small, q_r, q_g, q_y,
    wsem, zs, zr, xs, xr, ys, yr, fs, fr, qs, qr,
):
    nx, nz, nc, ny, cap = dims
    ng = nx * nc
    tok, width = x_ref.shape
    ff = up.shape[1]
    ch = ny
    cw = width // ch
    zrow, grow = ng * cap, nz * cap
    slots = nz * zrow
    e = lax.axis_index("expert")
    y = lax.axis_index("rep")
    x = e // (nz * nc)
    z = (e // nc) % nz
    c = e % nc
    g = x * nc + c

    def z_peer(k):
        zt = lax.rem(z + k, nz)
        return zt, ((x * nz + zt) * nc + c, y)

    def g_peer(k):
        gt = lax.rem(g + k, ng)
        return gt, (((gt // nc) * nz + z) * nc + gt % nc, y)

    def y_peer(k):
        yt = lax.rem(y + k, ny)
        return yt, (e, yt)

    load_up = pltpu.make_async_copy(up_hbm.at[0], up, wsem.at[0])
    load_down = pltpu.make_async_copy(down_hbm.at[0], down, wsem.at[1])

    barrier = pltpu.get_barrier_semaphore()
    peers = (
        [z_peer(k)[1] for k in range(1, nz)]
        + [g_peer(k)[1] for k in range(1, ng)]
        + [y_peer(k)[1] for k in range(1, ny)]
    )
    for peer in peers:
        pl.semaphore_signal(barrier, inc=1, device_id=peer, device_id_type=MESH)
    load_up.start()
    load_down.start()

    zorder = sorted(range(1, nz), key=lambda k: (-min(k, nz - k), k))
    gorder = sorted(range(1, ng), key=lambda k: (-min(k, ng - k), k))

    def z_send(st):
        for k in zorder:
            zt, dev = z_peer(k)
            pltpu.make_async_remote_copy(
                src_ref=sz.at[st, zt], dst_ref=rz.at[st, z],
                send_sem=zs.at[st], recv_sem=zr.at[st],
                device_id=dev, device_id_type=MESH,
            ).start()

    def g_send(st):
        for k in gorder:
            gt, dev = g_peer(k)
            pltpu.make_async_remote_copy(
                src_ref=sx.at[st, gt], dst_ref=rx.at[st, g],
                send_sem=xs.at[st], recv_sem=xr.at[st],
                device_id=dev, device_id_type=MESH,
            ).start()

    def wait_all(ref, st, count, sem):
        part = ref.at[st, pl.ds(0, count)]
        pltpu.make_async_copy(part, part, sem.at[st]).wait()

    def z_wait(st):
        wait_all(rz, st, nz - 1, zr)
        rz[st, z] = sz[st, z]

    def g_wait(st):
        wait_all(rx, st, ng - 1, xr)
        rx[st, g] = sx[st, g]

    def stage(kind, h):
        return "xrow".index(kind) * ch + h

    def ystage(kind, h):
        return "xrw".index(kind) * ch + h

    hg = ng // 2
    halves = (pl.ds(0, hg), pl.ds(hg, ng - hg))

    def y_copy(src, slot, sy, half, d, send, recv):
        _, dev = y_peer(1 if d == 0 else ny - 1)
        return pltpu.make_async_remote_copy(
            src_ref=src.at[halves[half]], dst_ref=ry.at[slot, sy, halves[half]],
            send_sem=send, recv_sem=recv, device_id=dev, device_id_type=MESH,
        )

    def y_home(kind, h, d, half):
        sy = ystage(kind, h)
        return y_copy(
            rx.at[stage(kind, h)], d, sy, half, d, ys.at[d, half, sy], yr.at[d, half, sy]
        )

    def y_hand(kind, h, d):
        sy = ystage(kind, h)
        return y_copy(ry.at[d, sy], 2, sy, d, d, fs.at[d, sy], fr.at[d, sy])

    def y_send(kind, h):
        for i in range(2):
            for d in range(2):
                y_home(kind, h, d, i if d == 0 else 1 - i).start()

    def y_relay(kind, h):
        for d in range(2):
            y_home(kind, h, d, d).wait_recv()
            y_hand(kind, h, d).start()

    def y_wait(kind, b, h):
        if b < 3:
            y_home(kind, h, b - 1, 2 - b).wait_recv()
        else:
            for d in range(2):
                y_hand(kind, h, d).wait_recv()

    def flatten(v):
        return v.astype(F32).reshape(slots, cw).astype(BF16)

    def put(ref, st, v):
        ref[st] = v.reshape(ref.shape[1:]).astype(BF16)

    def chunk(kind, b, h):
        if b == 0:
            return flatten(rx[stage(kind, 0) + h])
        return flatten(ry[b - 1, ystage(kind, 0) + h])

    def cols(h):
        return slice(h * cw, (h + 1) * cw)

    n_exp = nz * ng
    v = ids_ref[...]
    rest = v // nc
    q = (rest % nz) * ng + (rest // nz) * nc + v % nc
    small[0:2, :] = q.astype(F32)
    small[2:4, :] = gate_ref[...]
    small[4:8, :] = jnp.zeros((4, tok), F32)
    small_t = small[...].T
    col_e = lax.broadcasted_iota(jnp.int32, (tok, n_exp), 1).astype(F32)
    onehots = [jnp.where(col_e == small_t[:, k : k + 1], 1.0, 0.0).astype(F32) for k in range(2)]
    count = (onehots[0] + onehots[1]).astype(BF16)
    ti = lax.broadcasted_iota(jnp.int32, (tok, tok), 0)
    tj = lax.broadcasted_iota(jnp.int32, (tok, tok), 1)
    lower = jnp.where(tj < ti, 1.0, 0.0).astype(BF16)
    earlier = dot(lower, count)
    col_s = lax.broadcasted_iota(jnp.int32, (tok, slots), 1).astype(F32)
    for k in range(2):
        slot = jnp.sum(onehots[k] * earlier, axis=1, keepdims=True)
        pos = small_t[:, k : k + 1] * cap + slot
        m = jnp.where(col_s == pos, 1.0, 0.0).astype(F32)
        sel[k] = m.astype(BF16)
        selt[k] = m.T.astype(BF16)

    both = (selt[0].astype(F32) + selt[1].astype(F32)).astype(BF16)
    for h in range(ch):
        put(sz, stage("x", h), dot(both, x_ref[:, cols(h)]))
    pl.semaphore_wait(barrier, len(peers))
    for h in range(ch):
        z_send(stage("x", h))
    for h in range(ch):
        put(sz, stage("r", h), dot(both, r_ref[:, cols(h)]))
        z_send(stage("r", h))

    def forward(kind, h):
        st = stage(kind, h)
        z_wait(st)
        put(sx, st, dot(pf_ref[...], flatten(rz[st])))
        g_send(st)

    def arrive(kind, h):
        g_wait(stage(kind, h))
        y_send(kind, h)

    def gather(kind, b, first=0, last=ch):
        for h in range(first, last):
            act[b, :, cols(h)] = chunk(kind, b, h)

    def tiles(fn):
        @pl.loop(0, ff // TILE)
        def _(i):
            fn(pl.ds(pl.multiple_of(i * TILE, TILE), TILE))

    def pre_task(b):
        gather("x", b)
        xt[b] = chunk("x", b, y).astype(F32).T.astype(BF16)

        def fn(n):
            p = dot(act[b], up[:, n])
            s = 1.0 / (1.0 + jnp.exp(-p))
            sg[b, :, n] = s * (1.0 + p * (1.0 - s))
            pc[b, :, n] = s * (1.0 - s) * (2.0 + p * (1.0 - 2.0 * s))

        tiles(fn)

    def proj_done(b, n, p):
        scaled[b, :, n] = (sg[b, :, n] * p).astype(BF16)
        pc[b, :, n] = p * pc[b, :, n]

    def proj_task(b):
        gather("r", b)
        tiles(lambda n: proj_done(b, n, dot_t(act[b], down[n, :])))

    forward("x", 0)
    forward("x", 1)
    forward("x", 2)
    arrive("x", 0)
    forward("x", 3)
    arrive("x", 1)
    forward("r", 0)
    arrive("x", 2)
    y_relay("x", 0)
    forward("r", 1)
    arrive("x", 3)
    load_up.wait()
    load_down.wait()
    pre_task(0)
    forward("r", 2)
    arrive("r", 0)
    y_relay("x", 1)
    forward("r", 3)
    arrive("r", 1)
    y_relay("x", 2)
    part = (ch // 2) * cw
    gather("r", 0, 0, ch // 2)

    def early_proj(n):
        sg[1, :, n] = dot_t(act[0, :, :part], down[n, :part])

    tiles(early_proj)
    arrive("r", 2)
    arrive("r", 3)
    gather("r", 0, ch // 2, ch)
    tiles(lambda n: proj_done(
        0, n, sg[1, :, n] + dot_t(act[0, :, part:], down[n, part:])
    ))

    for h in range(ch):
        put(sx, stage("o", h), dot_t(scaled[0], up[cols(h), :]))
        g_send(stage("o", h))
    y_relay("x", 3)
    for h in range(ch):
        st = stage("o", h)
        g_wait(st)
        put(sz, st, dot(pb_ref[...], flatten(rx[st])))
        z_send(st)

    g0 = small[...].T[:, 2:3]
    g1 = small[...].T[:, 3:4]

    def combine(h):
        st = stage("o", h)
        z_wait(st)
        got = flatten(rz[st])
        ig = (
            r_ref[:, cols(h)].astype(F32)
            + g0 * dot(sel[0], got)
            + g1 * dot(sel[1], got)
        )
        cot = dot(selt[0], (g0 * ig).astype(BF16)) + dot(selt[1], (g1 * ig).astype(BF16))
        put(sz, stage("w", h), cot)
        z_send(stage("w", h))
        ig_ref[:, cols(h)] = ig
        return jnp.sum(ig * ig, axis=0, keepdims=True)

    y_relay("r", 0)
    for h in range(ch):
        y_wait("x", 1, h)
    pre_task(1)
    squares = combine(0)
    y_relay("r", 1)
    for h in range(ch):
        y_wait("x", 2, h)
    pre_task(2)
    squares = squares + combine(1)
    y_relay("r", 2)
    y_relay("r", 3)
    for h in range(ch):
        y_wait("r", 1, h)
    proj_task(1)
    squares = squares + combine(2)
    for h in range(ch):
        y_wait("r", 2, h)
    proj_task(2)
    squares = squares + combine(3)

    def q_send(buf, me, peer_of, n, st):
        for k in range(1, n):
            _, dev = peer_of(k)
            pltpu.make_async_remote_copy(
                src_ref=buf.at[me], dst_ref=buf.at[me],
                send_sem=qs.at[st], recv_sem=qr.at[st],
                device_id=dev, device_id_type=MESH,
            ).start()

    def q_wait(buf, n, st):
        some = buf.at[pl.ds(0, n - 1)]
        pltpu.make_async_copy(some, some, qr.at[st]).wait()
        pltpu.make_async_copy(some, some, qs.at[st]).wait()
        total = buf[0]
        for i in range(1, n):
            total = total + buf[i]
        return total

    lanes = q_r.shape[2]
    row = squares[:, :lanes]
    for i in range(1, cw // lanes):
        row = row + squares[:, i * lanes : (i + 1) * lanes]
    q_r[z] = jnp.broadcast_to(row * 0.125, q_r.shape[1:])
    q_send(q_r, z, z_peer, nz, 0)

    for h in range(ch):
        y_wait("x", 3, h)
    pre_task(3)
    forward("w", 0)
    for h in range(ch):
        y_wait("r", 3, h)
    proj_task(3)
    forward("w", 1)
    arrive("w", 0)
    q_g[g] = q_wait(q_r, nz, 0)
    q_send(q_g, g, g_peer, ng, 1)
    forward("w", 2)
    arrive("w", 1)
    forward("w", 3)
    arrive("w", 2)
    y_relay("w", 0)
    q_y[y] = q_wait(q_g, ng, 1)
    q_send(q_y, y, y_peer, ny, 2)
    arrive("w", 3)

    most = (ch - 1) * cw

    def early(b):
        gather("w", b, 0, ch - 1)

        def fn(n):
            sg[b, :, n] = dot(act[b, :, :most], up[:most, n])

        tiles(fn)

    def late(b):
        gather("w", b, ch - 1, ch)
        wt[b] = chunk("w", b, y).astype(F32).T.astype(BF16)

        def fn(n):
            s = sg[b, :, n] + dot(act[b, :, most:], up[most:, n])
            pre_grad = (s * pc[b, :, n]).astype(BF16)
            t = dot(wt[b], scaled[b, :, n]) + dot(xt[b], pre_grad)
            if b > 0:
                t = t + gacc[:, n]
            if b < 3:
                gacc[:, n] = t
            else:
                grad_ref[0, :, n] = t.astype(BF16)

        tiles(fn)

    early(0)
    y_relay("w", 1)
    late(0)
    y_relay("w", 2)
    for b in (1, 2):
        for h in range(ch - 1):
            y_wait("w", b, h)
    early(1)
    y_relay("w", 3)
    early(2)
    for b in (1, 2):
        y_wait("w", b, ch - 1)
        late(b)
    for h in range(ch - 1):
        y_wait("w", 3, h)
    early(3)
    y_wait("w", 3, ch - 1)
    late(3)

    total = q_wait(q_y, ny, 2)
    total = jnp.sum(jnp.sum(total, axis=0, keepdims=True), axis=1, keepdims=True)
    pen_ref[...] = jnp.broadcast_to(total, pen_ref.shape)

    for kind in "xrow":
        for h in range(ch):
            st = stage(kind, h)
            wait_all(sz, st, nz - 1, zs)
            wait_all(sx, st, ng - 1, xs)
            if kind != "o":
                for d in range(2):
                    y_home(kind, h, d, 0).wait_send()
                    y_home(kind, h, d, 1).wait_send()
                    y_hand(kind, h, d).wait_send()


def regroup(outer, inner, cap):
    n = outer * inner * cap
    src = np.arange(n).reshape(outer, inner, cap).transpose(1, 0, 2).reshape(-1)
    return jnp.asarray(np.eye(n, dtype=np.float32)[src], BF16)


def body(dims, features, readout, up_weight, down_weight, expert_ids, gate_values):
    nx, nz, nc, ny, cap = dims
    ng = nx * nc
    tok, width = features.shape
    ff = up_weight.shape[2]
    ch = ny
    cw = width // ch
    slots = nz * ng * cap
    lanes = min(cw, 128)
    vm = pl.BlockSpec(memory_space=pltpu.VMEM)
    hbm = pl.BlockSpec(memory_space=pl.ANY)
    dma = pltpu.SemaphoreType.DMA
    zbuf = pltpu.VMEM((4 * ch, nz, ng * cap, cw), BF16)
    gbuf = pltpu.VMEM((4 * ch, ng, nz * cap, cw), BF16)
    grad, ig, pen = pl.pallas_call(
        functools.partial(kernel, dims),
        out_shape=(
            jax.ShapeDtypeStruct((1, width // ny, ff), BF16),
            jax.ShapeDtypeStruct((tok, width), F32),
            jax.ShapeDtypeStruct((8, 128), F32),
        ),
        in_specs=[vm, vm, hbm, hbm, vm, vm, vm, vm],
        out_specs=(vm, vm, vm),
        scratch_shapes=[
            pltpu.VMEM((width, ff), BF16),
            pltpu.VMEM((ff, width), BF16),
            zbuf, zbuf, gbuf, gbuf,
            pltpu.VMEM((3, 3 * ch, ng, nz * cap, cw), BF16),
            pltpu.VMEM((4, slots, width), BF16),
            pltpu.VMEM((4, slots, ff), F32),
            pltpu.VMEM((4, slots, ff), F32),
            pltpu.VMEM((4, slots, ff), BF16),
            pltpu.VMEM((4, cw, slots), BF16),
            pltpu.VMEM((4, cw, slots), BF16),
            pltpu.VMEM((cw, ff), F32),
            pltpu.VMEM((2, tok, slots), BF16),
            pltpu.VMEM((2, slots, tok), BF16),
            pltpu.VMEM((8, tok), F32),
            pltpu.VMEM((nz, 8, lanes), F32),
            pltpu.VMEM((ng, 8, lanes), F32),
            pltpu.VMEM((ny, 8, lanes), F32),
            dma((2,)), dma((4 * ch,)), dma((4 * ch,)), dma((4 * ch,)), dma((4 * ch,)),
            dma((2, 2, 3 * ch)), dma((2, 2, 3 * ch)),
            dma((2, 3 * ch)), dma((2, 3 * ch)),
            dma((3,)), dma((3,)),
        ],
        compiler_params=pltpu.CompilerParams(
            collective_id=0, has_side_effects=True, vmem_limit_bytes=67043328
        ),
    )(
        features, readout, up_weight, down_weight, expert_ids.T, gate_values.T,
        regroup(nz, ng, cap), regroup(ng, nz, cap),
    )
    groups = nz * ng
    penalty = pen[0, 0] / (2.0 * tok * groups * ny * width)
    return grad, ig, penalty


def solution(mesh, dims=None):
    if dims is None:
        dims = (NX, NZ, NC, mesh.shape["rep"], CAP)
    both = ("expert", "rep")
    return jax.shard_map(
        functools.partial(body, dims),
        mesh=mesh,
        in_specs=(
            P(both, None), P(both, None),
            P("expert", None, None), P("expert", None, None),
            P(both, None), P(both, None),
        ),
        out_specs=(P("expert", "rep", None), P(both, None), P()),
        check_vma=False,
    )
```

```python
import functools

import jax
import jax.numpy as jnp
import numpy as np
from jax import lax
from jax.experimental import pallas as pl
from jax.experimental.pallas import tpu as pltpu
from jax.sharding import PartitionSpec as P

MESH = pl.DeviceIdType.MESH
F32 = jnp.float32
BF16 = jnp.bfloat16
NX, NZ, NC, CAP = 4, 8, 2, 5
TILE = 512


def dot(a, b):
    return lax.dot_general(a, b, (((1,), (0,)), ((), ())), preferred_element_type=F32)


def dot_t(a, b):
    return lax.dot_general(a, b, (((1,), (1,)), ((), ())), preferred_element_type=F32)


def kernel(
    dims,
    x_hbm, r_hbm, up_hbm, down_hbm, ids_hbm, gate_hbm, pf_hbm, pb_hbm,
    grad_hbm, ig_hbm, pen_hbm,
    x_ref, r_ref, ids_ref, gate_ref, pf_ref, pb_ref, grad_ref, ig_ref, pen_ref,
    up, down, sz, rz, sx, rx, ry, act, sg, pc, scaled, xt, wt, gacc,
    sel, selt, small, q_r, q_g, q_y,
    wsem, osem, zs, zr, xs, xr, ys, yr, fs, fr, qs, qr,
):
    nx, nz, nc, ny, cap = dims
    ng = nx * nc
    tok, width = x_ref.shape
    ff = up.shape[1]
    ch = ny
    cw = width // ch
    zrow, grow = ng * cap, nz * cap
    slots = nz * zrow
    e = lax.axis_index("expert")
    y = lax.axis_index("rep")
    x = e // (nz * nc)
    z = (e // nc) % nz
    c = e % nc
    g = x * nc + c

    def z_peer(k):
        zt = lax.rem(z + k, nz)
        return zt, ((x * nz + zt) * nc + c, y)

    def g_peer(k):
        gt = lax.rem(g + k, ng)
        return gt, (((gt // nc) * nz + z) * nc + gt % nc, y)

    def y_peer(k):
        yt = lax.rem(y + k, ny)
        return yt, (e, yt)

    barrier = pltpu.get_barrier_semaphore()
    peers = (
        [z_peer(k)[1] for k in range(1, nz)]
        + [g_peer(k)[1] for k in range(1, ng)]
        + [y_peer(k)[1] for k in range(1, ny)]
    )
    for peer in peers:
        pl.semaphore_signal(barrier, inc=1, device_id=peer, device_id_type=MESH)
    pairs = (
        (ids_hbm, ids_ref), (gate_hbm, gate_ref), (x_hbm, x_ref), (r_hbm, r_ref),
        (pf_hbm, pf_ref), (pb_hbm, pb_ref), (up_hbm.at[0], up), (down_hbm.at[0], down),
    )
    loads = [pltpu.make_async_copy(a, b, wsem.at[i]) for i, (a, b) in enumerate(pairs)]
    for load in loads:
        load.start()

    zorder = sorted(range(1, nz), key=lambda k: (-min(k, nz - k), k))
    gorder = sorted(range(1, ng), key=lambda k: (-min(k, ng - k), k))

    def z_send(st):
        for k in zorder:
            zt, dev = z_peer(k)
            pltpu.make_async_remote_copy(
                src_ref=sz.at[st, zt], dst_ref=rz.at[st, z],
                send_sem=zs.at[st], recv_sem=zr.at[st],
                device_id=dev, device_id_type=MESH,
            ).start()

    def g_send(st):
        for k in gorder:
            gt, dev = g_peer(k)
            pltpu.make_async_remote_copy(
                src_ref=sx.at[st, gt], dst_ref=rx.at[st, g],
                send_sem=xs.at[st], recv_sem=xr.at[st],
                device_id=dev, device_id_type=MESH,
            ).start()

    def wait_all(ref, st, count, sem):
        part = ref.at[st, pl.ds(0, count)]
        pltpu.make_async_copy(part, part, sem.at[st]).wait()

    def z_wait(st):
        wait_all(rz, st, nz - 1, zr)
        rz[st, z] = sz[st, z]

    def g_wait(st):
        wait_all(rx, st, ng - 1, xr)
        rx[st, g] = sx[st, g]

    def stage(kind, h):
        return "xrow".index(kind) * ch + h

    def ystage(kind, h):
        return "xrw".index(kind) * ch + h

    hg = ng // 2
    halves = (pl.ds(0, hg), pl.ds(hg, ng - hg))

    def y_copy(src, slot, sy, half, d, send, recv):
        _, dev = y_peer(1 if d == 0 else ny - 1)
        return pltpu.make_async_remote_copy(
            src_ref=src.at[halves[half]], dst_ref=ry.at[slot, sy, halves[half]],
            send_sem=send, recv_sem=recv, device_id=dev, device_id_type=MESH,
        )

    def y_home(kind, h, d, half):
        sy = ystage(kind, h)
        return y_copy(
            rx.at[stage(kind, h)], d, sy, half, d, ys.at[d, half, sy], yr.at[d, half, sy]
        )

    def y_hand(kind, h, d):
        sy = ystage(kind, h)
        return y_copy(ry.at[d, sy], 2, sy, d, d, fs.at[d, sy], fr.at[d, sy])

    def y_send(kind, h):
        for i in range(2):
            for d in range(2):
                y_home(kind, h, d, i if d == 0 else 1 - i).start()

    def y_relay(kind, h):
        for d in range(2):
            y_home(kind, h, d, d).wait_recv()
            y_hand(kind, h, d).start()

    def y_wait(kind, b, h):
        if b < 3:
            y_home(kind, h, b - 1, 2 - b).wait_recv()
        else:
            for d in range(2):
                y_hand(kind, h, d).wait_recv()

    def flatten(v):
        return v.astype(F32).reshape(slots, cw).astype(BF16)

    def put(ref, st, v):
        ref[st] = v.reshape(ref.shape[1:]).astype(BF16)

    def chunk(kind, b, h):
        if b == 0:
            return flatten(rx[stage(kind, 0) + h])
        return flatten(ry[b - 1, ystage(kind, 0) + h])

    def cols(h):
        return slice(h * cw, (h + 1) * cw)

    n_exp = nz * ng
    loads[0].wait()
    loads[1].wait()
    v = ids_ref[...]
    rest = v // nc
    q = (rest % nz) * ng + (rest // nz) * nc + v % nc
    small[0:2, :] = q.astype(F32)
    small[2:4, :] = gate_ref[...]
    small[4:8, :] = jnp.zeros((4, tok), F32)
    small_t = small[...].T
    col_e = lax.broadcasted_iota(jnp.int32, (tok, n_exp), 1).astype(F32)
    onehots = [jnp.where(col_e == small_t[:, k : k + 1], 1.0, 0.0).astype(F32) for k in range(2)]
    count = (onehots[0] + onehots[1]).astype(BF16)
    ti = lax.broadcasted_iota(jnp.int32, (tok, tok), 0)
    tj = lax.broadcasted_iota(jnp.int32, (tok, tok), 1)
    lower = jnp.where(tj < ti, 1.0, 0.0).astype(BF16)
    earlier = dot(lower, count)
    col_s = lax.broadcasted_iota(jnp.int32, (tok, slots), 1).astype(F32)
    for k in range(2):
        slot = jnp.sum(onehots[k] * earlier, axis=1, keepdims=True)
        pos = small_t[:, k : k + 1] * cap + slot
        m = jnp.where(col_s == pos, 1.0, 0.0).astype(F32)
        sel[k] = m.astype(BF16)
        selt[k] = m.T.astype(BF16)

    both = (selt[0].astype(F32) + selt[1].astype(F32)).astype(BF16)
    loads[2].wait()
    for h in range(ch):
        put(sz, stage("x", h), dot(both, x_ref[:, cols(h)]))
    pl.semaphore_wait(barrier, len(peers))
    for h in range(ch):
        z_send(stage("x", h))
    loads[3].wait()
    for h in range(ch):
        put(sz, stage("r", h), dot(both, r_ref[:, cols(h)]))
        z_send(stage("r", h))

    def forward(kind, h):
        st = stage(kind, h)
        z_wait(st)
        put(sx, st, dot(pf_ref[...], flatten(rz[st])))
        g_send(st)

    def arrive(kind, h):
        g_wait(stage(kind, h))
        y_send(kind, h)

    def gather(kind, b, first=0, last=ch):
        for h in range(first, last):
            act[b, :, cols(h)] = chunk(kind, b, h)

    def tiles(fn):
        @pl.loop(0, ff // TILE)
        def _(i):
            fn(pl.ds(pl.multiple_of(i * TILE, TILE), TILE))

    def pre_task(b):
        gather("x", b)
        xt[b] = chunk("x", b, y).astype(F32).T.astype(BF16)

        def fn(n):
            p = dot(act[b], up[:, n])
            s = 1.0 / (1.0 + jnp.exp(-p))
            sg[b, :, n] = s * (1.0 + p * (1.0 - s))
            pc[b, :, n] = s * (1.0 - s) * (2.0 + p * (1.0 - 2.0 * s))

        tiles(fn)

    def proj_done(b, n, p):
        scaled[b, :, n] = (sg[b, :, n] * p).astype(BF16)
        pc[b, :, n] = p * pc[b, :, n]

    def proj_task(b):
        gather("r", b)
        tiles(lambda n: proj_done(b, n, dot_t(act[b], down[n, :])))

    loads[4].wait()
    loads[5].wait()
    forward("x", 0)
    forward("x", 1)
    forward("x", 2)
    arrive("x", 0)
    forward("x", 3)
    arrive("x", 1)
    forward("r", 0)
    arrive("x", 2)
    y_relay("x", 0)
    forward("r", 1)
    arrive("x", 3)
    loads[6].wait()
    loads[7].wait()
    pre_task(0)
    forward("r", 2)
    arrive("r", 0)
    y_relay("x", 1)
    forward("r", 3)
    arrive("r", 1)
    y_relay("x", 2)
    part = (ch // 2) * cw
    gather("r", 0, 0, ch // 2)

    def early_proj(n):
        sg[1, :, n] = dot_t(act[0, :, :part], down[n, :part])

    tiles(early_proj)
    arrive("r", 2)
    arrive("r", 3)
    gather("r", 0, ch // 2, ch)
    tiles(lambda n: proj_done(
        0, n, sg[1, :, n] + dot_t(act[0, :, part:], down[n, part:])
    ))

    for h in range(ch):
        put(sx, stage("o", h), dot_t(scaled[0], up[cols(h), :]))
        g_send(stage("o", h))

    def back(h):
        st = stage("o", h)
        g_wait(st)
        put(sz, st, dot(pb_ref[...], flatten(rx[st])))

    back(0)
    z_send(stage("o", 0))
    back(1)
    z_send(stage("o", 1))

    g0 = small[...].T[:, 2:3]
    g1 = small[...].T[:, 3:4]

    def combine(h):
        st = stage("o", h)
        z_wait(st)
        got = flatten(rz[st])
        ig = (
            r_ref[:, cols(h)].astype(F32)
            + g0 * dot(sel[0], got)
            + g1 * dot(sel[1], got)
        )
        cot = dot(selt[0], (g0 * ig).astype(BF16)) + dot(selt[1], (g1 * ig).astype(BF16))
        put(sz, stage("w", h), cot)
        z_send(stage("w", h))
        ig_ref[:, cols(h)] = ig
        return jnp.sum(ig * ig, axis=0, keepdims=True)

    def y_all(kind, b):
        for h in range(ch):
            y_wait(kind, b, h)

    y_relay("x", 3)
    y_relay("r", 0)
    y_all("x", 1)
    pre_task(1)
    back(2)
    back(3)
    squares = combine(0)
    z_send(stage("o", 2))
    y_relay("r", 1)
    y_all("x", 2)
    pre_task(2)
    squares = squares + combine(1)
    z_send(stage("o", 3))
    y_relay("r", 2)
    forward("w", 0)
    y_relay("r", 3)
    y_all("r", 1)
    proj_task(1)
    squares = squares + combine(2)
    arrive("w", 0)
    y_all("r", 2)
    proj_task(2)
    forward("w", 1)
    squares = squares + combine(3)
    save_ig = pltpu.make_async_copy(ig_ref, ig_hbm, osem.at[1])
    save_ig.start()
    arrive("w", 1)

    def q_send(buf, me, peer_of, n, st):
        for k in range(1, n):
            _, dev = peer_of(k)
            pltpu.make_async_remote_copy(
                src_ref=buf.at[me], dst_ref=buf.at[me],
                send_sem=qs.at[st], recv_sem=qr.at[st],
                device_id=dev, device_id_type=MESH,
            ).start()

    def q_wait(buf, n, st):
        some = buf.at[pl.ds(0, n - 1)]
        pltpu.make_async_copy(some, some, qr.at[st]).wait()
        pltpu.make_async_copy(some, some, qs.at[st]).wait()
        total = buf[0]
        for i in range(1, n):
            total = total + buf[i]
        return total

    lanes = q_r.shape[2]
    row = squares[:, :lanes]
    for i in range(1, cw // lanes):
        row = row + squares[:, i * lanes : (i + 1) * lanes]
    q_r[z] = jnp.broadcast_to(row * 0.125, q_r.shape[1:])
    q_send(q_r, z, z_peer, nz, 0)

    y_all("x", 3)
    pre_task(3)
    y_relay("w", 0)
    forward("w", 2)
    q_g[g] = q_wait(q_r, nz, 0)
    q_send(q_g, g, g_peer, ng, 1)
    y_all("r", 3)
    proj_task(3)
    forward("w", 3)
    arrive("w", 2)
    y_relay("w", 1)

    most = (ch - 1) * cw

    def early(b):
        gather("w", b, 0, ch - 1)

        def fn(n):
            sg[b, :, n] = dot(act[b, :, :most], up[:most, n])

        tiles(fn)

    def late(b):
        gather("w", b, ch - 1, ch)
        wt[b] = chunk("w", b, y).astype(F32).T.astype(BF16)

        def fn(n):
            s = sg[b, :, n] + dot(act[b, :, most:], up[most:, n])
            pre_grad = (s * pc[b, :, n]).astype(BF16)
            t = dot(wt[b], scaled[b, :, n]) + dot(xt[b], pre_grad)
            if b > 0:
                t = t + gacc[:, n]
            if b < 3:
                gacc[:, n] = t
            else:
                grad_ref[0, :, n] = t.astype(BF16)
                pltpu.make_async_copy(
                    grad_ref.at[:, :, n], grad_hbm.at[:, :, n], osem.at[0]
                ).start()

        tiles(fn)

    early(0)
    q_y[y] = q_wait(q_g, ng, 1)
    q_send(q_y, y, y_peer, ny, 2)
    arrive("w", 3)
    y_relay("w", 2)
    late(0)
    for b in (1, 2):
        for h in range(ch - 1):
            y_wait("w", b, h)
        early(b)
        if b == 1:
            y_relay("w", 3)
    for b in (1, 2):
        y_wait("w", b, ch - 1)
        late(b)
    for h in range(ch - 1):
        y_wait("w", 3, h)
    early(3)
    total = q_wait(q_y, ny, 2)
    total = jnp.sum(jnp.sum(total, axis=0, keepdims=True), axis=1, keepdims=True)
    pen_ref[...] = jnp.broadcast_to(total, pen_ref.shape)
    save_pen = pltpu.make_async_copy(pen_ref, pen_hbm, osem.at[2])
    save_pen.start()
    y_wait("w", 3, ch - 1)
    late(3)

    for kind in "xrow":
        for h in range(ch):
            st = stage(kind, h)
            wait_all(sz, st, nz - 1, zs)
            wait_all(sx, st, ng - 1, xs)
            if kind != "o":
                for d in range(2):
                    y_home(kind, h, d, 0).wait_send()
                    y_home(kind, h, d, 1).wait_send()
                    y_hand(kind, h, d).wait_send()
    pltpu.make_async_copy(grad_ref, grad_hbm, osem.at[0]).wait()
    save_ig.wait()
    save_pen.wait()


def finish(scale, grad_in, ig_in, pen_in, grad_out, ig_out, pen_out, gbuf, ibuf, isem, osem):
    steps = []
    parts = 2
    for i in range(parts):
        n = grad_in.shape[1] // parts
        steps.append((grad_in, gbuf, grad_out, (slice(None), pl.ds(i * n, n))))
    steps.append((ig_in, ibuf, ig_out, (slice(None),)))
    reads = [
        pltpu.make_async_copy(a.at[at], v.at[at], isem.at[i])
        for i, (a, v, b, at) in enumerate(steps)
    ]
    writes = [
        pltpu.make_async_copy(v.at[at], b.at[at], osem.at[i])
        for i, (a, v, b, at) in enumerate(steps)
    ]
    for read in reads:
        read.start()
    pen_out[...] = pen_in[0:1, 0:1] * scale
    for read, write in zip(reads, writes):
        read.wait()
        write.start()
    for write in writes:
        write.wait()


def regroup(outer, inner, cap):
    n = outer * inner * cap
    src = np.arange(n).reshape(outer, inner, cap).transpose(1, 0, 2).reshape(-1)
    return jnp.asarray(np.eye(n, dtype=np.float32)[src], BF16)


def body(dims, features, readout, up_weight, down_weight, expert_ids, gate_values):
    nx, nz, nc, ny, cap = dims
    ng = nx * nc
    tok, width = features.shape
    ff = up_weight.shape[2]
    ch = ny
    cw = width // ch
    slots = nz * ng * cap
    lanes = min(cw, 128)
    vm = pl.BlockSpec(memory_space=pltpu.VMEM)
    hbm = pl.BlockSpec(memory_space=pl.ANY)
    dma = pltpu.SemaphoreType.DMA
    zbuf = pltpu.VMEM((4 * ch, nz, ng * cap, cw), BF16)
    gbuf = pltpu.VMEM((4 * ch, ng, nz * cap, cw), BF16)
    grad, ig, pen = pl.pallas_call(
        functools.partial(kernel, dims),
        out_shape=(
            jax.ShapeDtypeStruct((1, width // ny, ff), BF16),
            jax.ShapeDtypeStruct((tok, width), F32),
            jax.ShapeDtypeStruct((8, 128), F32),
        ),
        in_specs=[hbm] * 8,
        out_specs=(hbm, hbm, hbm),
        scratch_shapes=[
            pltpu.VMEM((tok, width), BF16),
            pltpu.VMEM((tok, width), BF16),
            pltpu.VMEM((2, tok), jnp.int32),
            pltpu.VMEM((2, tok), F32),
            pltpu.VMEM((slots, slots), BF16),
            pltpu.VMEM((slots, slots), BF16),
            pltpu.VMEM((1, width // ny, ff), BF16),
            pltpu.VMEM((tok, width), F32),
            pltpu.VMEM((8, 128), F32),
            pltpu.VMEM((width, ff), BF16),
            pltpu.VMEM((ff, width), BF16),
            zbuf, zbuf, gbuf, gbuf,
            pltpu.VMEM((3, 3 * ch, ng, nz * cap, cw), BF16),
            pltpu.VMEM((4, slots, width), BF16),
            pltpu.VMEM((4, slots, ff), F32),
            pltpu.VMEM((4, slots, ff), F32),
            pltpu.VMEM((4, slots, ff), BF16),
            pltpu.VMEM((4, cw, slots), BF16),
            pltpu.VMEM((4, cw, slots), BF16),
            pltpu.VMEM((cw, ff), F32),
            pltpu.VMEM((2, tok, slots), BF16),
            pltpu.VMEM((2, slots, tok), BF16),
            pltpu.VMEM((8, tok), F32),
            pltpu.VMEM((nz, 8, lanes), F32),
            pltpu.VMEM((ng, 8, lanes), F32),
            pltpu.VMEM((ny, 8, lanes), F32),
            dma((8,)), dma((3,)), dma((4 * ch,)), dma((4 * ch,)), dma((4 * ch,)), dma((4 * ch,)),
            dma((2, 2, 3 * ch)), dma((2, 2, 3 * ch)),
            dma((2, 3 * ch)), dma((2, 3 * ch)),
            dma((3,)), dma((3,)),
        ],
        compiler_params=pltpu.CompilerParams(
            collective_id=0, has_side_effects=True, vmem_limit_bytes=67043328
        ),
    )(
        features, readout, up_weight, down_weight, expert_ids.T, gate_values.T,
        regroup(nz, ng, cap), regroup(ng, nz, cap),
    )
    scale = 1.0 / (2.0 * tok * nz * ng * ny * width)
    grad, ig, pen = pl.pallas_call(
        functools.partial(finish, scale),
        out_shape=(
            jax.ShapeDtypeStruct(grad.shape, BF16),
            jax.ShapeDtypeStruct(ig.shape, F32),
            jax.ShapeDtypeStruct((1, 1), F32),
        ),
        in_specs=[hbm, hbm, vm],
        out_specs=(hbm, hbm, vm),
        scratch_shapes=[
            pltpu.VMEM(grad.shape, BF16), pltpu.VMEM(ig.shape, F32), dma((3,)), dma((3,)),
        ],
        compiler_params=pltpu.CompilerParams(vmem_limit_bytes=67043328),
    )(grad, ig, pen)
    return grad, ig, pen.reshape(())


def solution(mesh, dims=None):
    if dims is None:
        dims = (NX, NZ, NC, mesh.shape["rep"], CAP)
    both = ("expert", "rep")
    return jax.shard_map(
        functools.partial(body, dims),
        mesh=mesh,
        in_specs=(
            P(both, None), P(both, None),
            P("expert", None, None), P("expert", None, None),
            P(both, None), P(both, None),
        ),
        out_specs=(P("expert", "rep", None), P(both, None), P()),
        check_vma=False,
    )
```

```python
import functools

import jax
import jax.numpy as jnp
import numpy as np
from jax import lax
from jax.experimental import pallas as pl
from jax.experimental.pallas import tpu as pltpu
from jax.sharding import PartitionSpec as P

MESH = pl.DeviceIdType.MESH
F32 = jnp.float32
BF16 = jnp.bfloat16
NX, NZ, NC, CAP = 4, 8, 2, 5
TILE = 1024


def dot(a, b):
    return lax.dot_general(a, b, (((1,), (0,)), ((), ())), preferred_element_type=F32)


def dot_t(a, b):
    return lax.dot_general(a, b, (((1,), (1,)), ((), ())), preferred_element_type=F32)


def kernel(
    dims,
    x_hbm, r_hbm, up_hbm, down_hbm, ids_hbm, gate_hbm, pf_hbm, pb_hbm,
    grad_hbm, ig_hbm, pen_hbm,
    x_ref, r_ref, ids_ref, gate_ref, pf_ref, pb_ref, grad_ref, ig_ref, pen_ref,
    up, down, sz, rz, sx, rx, ry, act, sg, pc, scaled, xt, wt, gacc,
    sel, selt, small, q_r, q_g, q_y,
    wsem, osem, zs, zr, xs, xr, ys, yr, fs, fr, qs, qr,
):
    nx, nz, nc, ny, cap = dims
    ng = nx * nc
    tok, width = x_ref.shape
    ff = up.shape[1]
    ch = ny
    cw = width // ch
    zrow, grow = ng * cap, nz * cap
    slots = nz * zrow
    e = lax.axis_index("expert")
    y = lax.axis_index("rep")
    x = e // (nz * nc)
    z = (e // nc) % nz
    c = e % nc
    g = x * nc + c

    def z_peer(k):
        zt = lax.rem(z + k, nz)
        return zt, ((x * nz + zt) * nc + c, y)

    def g_peer(k):
        gt = lax.rem(g + k, ng)
        return gt, (((gt // nc) * nz + z) * nc + gt % nc, y)

    def y_peer(k):
        yt = lax.rem(y + k, ny)
        return yt, (e, yt)

    barrier = pltpu.get_barrier_semaphore()
    peers = (
        [z_peer(k)[1] for k in range(1, nz)]
        + [g_peer(k)[1] for k in range(1, ng)]
        + [y_peer(k)[1] for k in range(1, ny)]
    )
    for peer in peers:
        pl.semaphore_signal(barrier, inc=1, device_id=peer, device_id_type=MESH)
    pairs = (
        (ids_hbm, ids_ref), (gate_hbm, gate_ref), (x_hbm, x_ref), (r_hbm, r_ref),
        (pf_hbm, pf_ref), (pb_hbm, pb_ref), (up_hbm.at[0], up), (down_hbm.at[0], down),
    )
    loads = [pltpu.make_async_copy(a, b, wsem.at[i]) for i, (a, b) in enumerate(pairs)]
    for load in loads:
        load.start()

    zorder = sorted(range(1, nz), key=lambda k: (-min(k, nz - k), k))
    gorder = sorted(range(1, ng), key=lambda k: (-min(k, ng - k), k))

    def z_send(st):
        for k in zorder:
            zt, dev = z_peer(k)
            pltpu.make_async_remote_copy(
                src_ref=sz.at[st, zt], dst_ref=rz.at[st, z],
                send_sem=zs.at[st], recv_sem=zr.at[st],
                device_id=dev, device_id_type=MESH,
            ).start()

    def g_send(st):
        for k in gorder:
            gt, dev = g_peer(k)
            pltpu.make_async_remote_copy(
                src_ref=sx.at[st, gt], dst_ref=rx.at[st, g],
                send_sem=xs.at[st], recv_sem=xr.at[st],
                device_id=dev, device_id_type=MESH,
            ).start()

    def wait_all(ref, st, count, sem):
        part = ref.at[st, pl.ds(0, count)]
        pltpu.make_async_copy(part, part, sem.at[st]).wait()

    def z_wait(st):
        wait_all(rz, st, nz - 1, zr)
        rz[st, z] = sz[st, z]

    def g_wait(st):
        wait_all(rx, st, ng - 1, xr)
        rx[st, g] = sx[st, g]

    def stage(kind, h):
        return "xrow".index(kind) * ch + h

    def ystage(kind, h):
        return "xrw".index(kind) * ch + h

    hg = ng // 2
    halves = (pl.ds(0, hg), pl.ds(hg, ng - hg))

    def y_copy(src, slot, sy, half, d, send, recv):
        _, dev = y_peer(1 if d == 0 else ny - 1)
        return pltpu.make_async_remote_copy(
            src_ref=src.at[halves[half]], dst_ref=ry.at[slot, sy, halves[half]],
            send_sem=send, recv_sem=recv, device_id=dev, device_id_type=MESH,
        )

    def y_home(kind, h, d, half):
        sy = ystage(kind, h)
        return y_copy(
            rx.at[stage(kind, h)], d, sy, half, d, ys.at[d, half, sy], yr.at[d, half, sy]
        )

    def y_hand(kind, h, d):
        sy = ystage(kind, h)
        return y_copy(ry.at[d, sy], 2, sy, d, d, fs.at[d, sy], fr.at[d, sy])

    def y_send(kind, h):
        for i in range(2):
            for d in range(2):
                y_home(kind, h, d, i if d == 0 else 1 - i).start()

    def y_relay(kind, h):
        for d in range(2):
            y_home(kind, h, d, d).wait_recv()
            y_hand(kind, h, d).start()

    def y_wait(kind, b, h):
        if b < 3:
            y_home(kind, h, b - 1, 2 - b).wait_recv()
        else:
            for d in range(2):
                y_hand(kind, h, d).wait_recv()

    def flatten(v):
        return v.astype(F32).reshape(slots, cw).astype(BF16)

    def put(ref, st, v):
        ref[st] = v.reshape(ref.shape[1:]).astype(BF16)

    def chunk(kind, b, h):
        if b == 0:
            return flatten(rx[stage(kind, 0) + h])
        return flatten(ry[b - 1, ystage(kind, 0) + h])

    def cols(h):
        return slice(h * cw, (h + 1) * cw)

    n_exp = nz * ng
    loads[0].wait()
    loads[1].wait()
    v = ids_ref[...]
    rest = v // nc
    q = (rest % nz) * ng + (rest // nz) * nc + v % nc
    small[0:2, :] = q.astype(F32)
    small[2:4, :] = gate_ref[...]
    small[4:8, :] = jnp.zeros((4, tok), F32)
    small_t = small[...].T
    col_e = lax.broadcasted_iota(jnp.int32, (tok, n_exp), 1).astype(F32)
    onehots = [jnp.where(col_e == small_t[:, k : k + 1], 1.0, 0.0).astype(F32) for k in range(2)]
    count = (onehots[0] + onehots[1]).astype(BF16)
    ti = lax.broadcasted_iota(jnp.int32, (tok, tok), 0)
    tj = lax.broadcasted_iota(jnp.int32, (tok, tok), 1)
    lower = jnp.where(tj < ti, 1.0, 0.0).astype(BF16)
    earlier = dot(lower, count)
    col_s = lax.broadcasted_iota(jnp.int32, (tok, slots), 1).astype(F32)
    for k in range(2):
        slot = jnp.sum(onehots[k] * earlier, axis=1, keepdims=True)
        pos = small_t[:, k : k + 1] * cap + slot
        m = jnp.where(col_s == pos, 1.0, 0.0).astype(F32)
        sel[k] = m.astype(BF16)
        selt[k] = m.T.astype(BF16)

    both = (selt[0].astype(F32) + selt[1].astype(F32)).astype(BF16)
    loads[2].wait()
    for h in range(ch):
        put(sz, stage("x", h), dot(both, x_ref[:, cols(h)]))
    pl.semaphore_wait(barrier, len(peers))
    for h in range(ch):
        z_send(stage("x", h))
    loads[3].wait()
    for h in range(ch):
        put(sz, stage("r", h), dot(both, r_ref[:, cols(h)]))
        z_send(stage("r", h))

    def forward(kind, h):
        st = stage(kind, h)
        z_wait(st)
        put(sx, st, dot(pf_ref[...], flatten(rz[st])))
        g_send(st)

    def arrive(kind, h):
        g_wait(stage(kind, h))
        y_send(kind, h)

    def gather(kind, b, first=0, last=ch):
        for h in range(first, last):
            act[b, :, cols(h)] = chunk(kind, b, h)

    def tiles(fn):
        @pl.loop(0, ff // TILE)
        def _(i):
            fn(pl.ds(pl.multiple_of(i * TILE, TILE), TILE))

    def pre_task(b):
        gather("x", b)
        xt[b] = chunk("x", b, y).astype(F32).T.astype(BF16)

        def fn(n):
            p = dot(act[b], up[:, n])
            s = 1.0 / (1.0 + jnp.exp(-p))
            sg[b, :, n] = s * (1.0 + p * (1.0 - s))
            pc[b, :, n] = s * (1.0 - s) * (2.0 + p * (1.0 - 2.0 * s))

        tiles(fn)

    def proj_done(b, n, p):
        scaled[b, :, n] = (sg[b, :, n] * p).astype(BF16)
        pc[b, :, n] = p * pc[b, :, n]

    def proj_task(b):
        gather("r", b)
        tiles(lambda n: proj_done(b, n, dot_t(act[b], down[n, :])))

    loads[4].wait()
    loads[5].wait()
    forward("x", 0)
    forward("x", 1)
    forward("x", 2)
    arrive("x", 0)
    forward("x", 3)
    arrive("x", 1)
    forward("r", 0)
    arrive("x", 2)
    y_relay("x", 0)
    forward("r", 1)
    arrive("x", 3)
    loads[6].wait()
    loads[7].wait()
    pre_task(0)
    forward("r", 2)
    arrive("r", 0)
    y_relay("x", 1)
    forward("r", 3)
    arrive("r", 1)
    y_relay("x", 2)
    part = (ch - 1) * cw
    arrive("r", 2)
    gather("r", 0, 0, ch - 1)

    def early_proj(n):
        sg[1, :, n] = dot_t(act[0, :, :part], down[n, :part])

    tiles(early_proj)
    arrive("r", 3)
    gather("r", 0, ch - 1, ch)
    tiles(lambda n: proj_done(
        0, n, sg[1, :, n] + dot_t(act[0, :, part:], down[n, part:])
    ))

    for h in range(ch):
        put(sx, stage("o", h), dot_t(scaled[0], up[cols(h), :]))
        g_send(stage("o", h))

    def back(h):
        st = stage("o", h)
        g_wait(st)
        put(sz, st, dot(pb_ref[...], flatten(rx[st])))

    back(0)
    z_send(stage("o", 0))
    back(1)
    z_send(stage("o", 1))

    g0 = small[...].T[:, 2:3]
    g1 = small[...].T[:, 3:4]

    def combine(h):
        st = stage("o", h)
        z_wait(st)
        got = flatten(rz[st])
        ig = (
            r_ref[:, cols(h)].astype(F32)
            + g0 * dot(sel[0], got)
            + g1 * dot(sel[1], got)
        )
        cot = dot(selt[0], (g0 * ig).astype(BF16)) + dot(selt[1], (g1 * ig).astype(BF16))
        put(sz, stage("w", h), cot)
        z_send(stage("w", h))
        ig_ref[:, cols(h)] = ig
        return jnp.sum(ig * ig, axis=0, keepdims=True)

    def y_all(kind, b):
        for h in range(ch):
            y_wait(kind, b, h)

    y_relay("x", 3)
    y_relay("r", 0)
    y_all("x", 1)
    pre_task(1)
    back(2)
    back(3)
    squares = combine(0)
    z_send(stage("o", 2))
    y_relay("r", 1)
    y_all("x", 2)
    pre_task(2)
    squares = squares + combine(1)
    z_send(stage("o", 3))
    y_relay("r", 2)
    forward("w", 0)
    y_relay("r", 3)
    y_all("r", 1)
    proj_task(1)
    squares = squares + combine(2)
    arrive("w", 0)
    y_all("r", 2)
    proj_task(2)
    forward("w", 1)
    squares = squares + combine(3)
    save_ig = pltpu.make_async_copy(ig_ref, ig_hbm, osem.at[1])
    save_ig.start()
    arrive("w", 1)

    def q_send(buf, me, peer_of, n, st):
        for k in range(1, n):
            _, dev = peer_of(k)
            pltpu.make_async_remote_copy(
                src_ref=buf.at[me], dst_ref=buf.at[me],
                send_sem=qs.at[st], recv_sem=qr.at[st],
                device_id=dev, device_id_type=MESH,
            ).start()

    def q_wait(buf, n, st):
        some = buf.at[pl.ds(0, n - 1)]
        pltpu.make_async_copy(some, some, qr.at[st]).wait()
        pltpu.make_async_copy(some, some, qs.at[st]).wait()
        total = buf[0]
        for i in range(1, n):
            total = total + buf[i]
        return total

    lanes = q_r.shape[2]
    row = squares[:, :lanes]
    for i in range(1, cw // lanes):
        row = row + squares[:, i * lanes : (i + 1) * lanes]
    q_r[z] = jnp.broadcast_to(row * 0.125, q_r.shape[1:])
    q_send(q_r, z, z_peer, nz, 0)

    y_all("x", 3)
    pre_task(3)
    y_relay("w", 0)
    forward("w", 2)
    q_g[g] = q_wait(q_r, nz, 0)
    q_send(q_g, g, g_peer, ng, 1)
    y_all("r", 3)
    proj_task(3)
    forward("w", 3)
    arrive("w", 2)
    y_relay("w", 1)

    most = (ch - 1) * cw

    def early(b):
        gather("w", b, 0, ch - 1)

        def fn(n):
            sg[b, :, n] = dot(act[b, :, :most], up[:most, n])

        tiles(fn)

    def late(b):
        gather("w", b, ch - 1, ch)
        wt[b] = chunk("w", b, y).astype(F32).T.astype(BF16)

        def fn(n):
            s = sg[b, :, n] + dot(act[b, :, most:], up[most:, n])
            pre_grad = (s * pc[b, :, n]).astype(BF16)
            t = dot(wt[b], scaled[b, :, n]) + dot(xt[b], pre_grad)
            if b > 0:
                t = t + gacc[:, n]
            if b < 3:
                gacc[:, n] = t
            else:
                grad_ref[0, :, n] = t.astype(BF16)
                pltpu.make_async_copy(
                    grad_ref.at[:, :, n], grad_hbm.at[:, :, n], osem.at[0]
                ).start()

        tiles(fn)

    early(0)
    q_y[y] = q_wait(q_g, ng, 1)
    q_send(q_y, y, y_peer, ny, 2)
    arrive("w", 3)
    y_relay("w", 2)
    late(0)
    for b in (1, 2):
        for h in range(ch - 1):
            y_wait("w", b, h)
        early(b)
        if b == 1:
            y_relay("w", 3)
    for b in (1, 2):
        y_wait("w", b, ch - 1)
        late(b)
    for h in range(ch - 1):
        y_wait("w", 3, h)
    early(3)
    total = q_wait(q_y, ny, 2)
    total = jnp.sum(jnp.sum(total, axis=0, keepdims=True), axis=1, keepdims=True)
    pen_ref[...] = jnp.broadcast_to(total, pen_ref.shape)
    save_pen = pltpu.make_async_copy(pen_ref, pen_hbm, osem.at[2])
    save_pen.start()
    y_wait("w", 3, ch - 1)
    late(3)

    for kind in "xrow":
        for h in range(ch):
            st = stage(kind, h)
            wait_all(sz, st, nz - 1, zs)
            wait_all(sx, st, ng - 1, xs)
            if kind != "o":
                for d in range(2):
                    y_home(kind, h, d, 0).wait_send()
                    y_home(kind, h, d, 1).wait_send()
                    y_hand(kind, h, d).wait_send()
    pltpu.make_async_copy(grad_ref, grad_hbm, osem.at[0]).wait()
    save_ig.wait()
    save_pen.wait()


def finish(scale, grad_in, ig_in, pen_in, grad_out, ig_out, pen_out, gbuf, ibuf, isem, osem):
    steps = []
    parts = 2
    for i in range(parts):
        n = grad_in.shape[1] // parts
        steps.append((grad_in, gbuf, grad_out, (slice(None), pl.ds(i * n, n))))
    steps.append((ig_in, ibuf, ig_out, (slice(None),)))
    reads = [
        pltpu.make_async_copy(a.at[at], v.at[at], isem.at[i])
        for i, (a, v, b, at) in enumerate(steps)
    ]
    writes = [
        pltpu.make_async_copy(v.at[at], b.at[at], osem.at[i])
        for i, (a, v, b, at) in enumerate(steps)
    ]
    for read in reads:
        read.start()
    pen_out[...] = pen_in[0:1, 0:1] * scale
    for read, write in zip(reads, writes):
        read.wait()
        write.start()
    for write in writes:
        write.wait()


def regroup(outer, inner, cap):
    n = outer * inner * cap
    src = np.arange(n).reshape(outer, inner, cap).transpose(1, 0, 2).reshape(-1)
    return jnp.asarray(np.eye(n, dtype=np.float32)[src], BF16)


def body(dims, features, readout, up_weight, down_weight, expert_ids, gate_values):
    nx, nz, nc, ny, cap = dims
    ng = nx * nc
    tok, width = features.shape
    ff = up_weight.shape[2]
    ch = ny
    cw = width // ch
    slots = nz * ng * cap
    lanes = min(cw, 128)
    vm = pl.BlockSpec(memory_space=pltpu.VMEM)
    hbm = pl.BlockSpec(memory_space=pl.ANY)
    dma = pltpu.SemaphoreType.DMA
    zbuf = pltpu.VMEM((4 * ch, nz, ng * cap, cw), BF16)
    gbuf = pltpu.VMEM((4 * ch, ng, nz * cap, cw), BF16)
    grad, ig, pen = pl.pallas_call(
        functools.partial(kernel, dims),
        out_shape=(
            jax.ShapeDtypeStruct((1, width // ny, ff), BF16),
            jax.ShapeDtypeStruct((tok, width), F32),
            jax.ShapeDtypeStruct((8, 128), F32),
        ),
        in_specs=[hbm] * 8,
        out_specs=(hbm, hbm, hbm),
        scratch_shapes=[
            pltpu.VMEM((tok, width), BF16),
            pltpu.VMEM((tok, width), BF16),
            pltpu.VMEM((2, tok), jnp.int32),
            pltpu.VMEM((2, tok), F32),
            pltpu.VMEM((slots, slots), BF16),
            pltpu.VMEM((slots, slots), BF16),
            pltpu.VMEM((1, width // ny, ff), BF16),
            pltpu.VMEM((tok, width), F32),
            pltpu.VMEM((8, 128), F32),
            pltpu.VMEM((width, ff), BF16),
            pltpu.VMEM((ff, width), BF16),
            zbuf, zbuf, gbuf, gbuf,
            pltpu.VMEM((3, 3 * ch, ng, nz * cap, cw), BF16),
            pltpu.VMEM((4, slots, width), BF16),
            pltpu.VMEM((4, slots, ff), F32),
            pltpu.VMEM((4, slots, ff), F32),
            pltpu.VMEM((4, slots, ff), BF16),
            pltpu.VMEM((4, cw, slots), BF16),
            pltpu.VMEM((4, cw, slots), BF16),
            pltpu.VMEM((cw, ff), F32),
            pltpu.VMEM((2, tok, slots), BF16),
            pltpu.VMEM((2, slots, tok), BF16),
            pltpu.VMEM((8, tok), F32),
            pltpu.VMEM((nz, 8, lanes), F32),
            pltpu.VMEM((ng, 8, lanes), F32),
            pltpu.VMEM((ny, 8, lanes), F32),
            dma((8,)), dma((3,)), dma((4 * ch,)), dma((4 * ch,)), dma((4 * ch,)), dma((4 * ch,)),
            dma((2, 2, 3 * ch)), dma((2, 2, 3 * ch)),
            dma((2, 3 * ch)), dma((2, 3 * ch)),
            dma((3,)), dma((3,)),
        ],
        compiler_params=pltpu.CompilerParams(
            collective_id=0, has_side_effects=True, vmem_limit_bytes=67043328
        ),
    )(
        features, readout, up_weight, down_weight, expert_ids.T, gate_values.T,
        regroup(nz, ng, cap), regroup(ng, nz, cap),
    )
    scale = 1.0 / (2.0 * tok * nz * ng * ny * width)
    grad, ig, pen = pl.pallas_call(
        functools.partial(finish, scale),
        out_shape=(
            jax.ShapeDtypeStruct(grad.shape, BF16),
            jax.ShapeDtypeStruct(ig.shape, F32),
            jax.ShapeDtypeStruct((1, 1), F32),
        ),
        in_specs=[hbm, hbm, vm],
        out_specs=(hbm, hbm, vm),
        scratch_shapes=[
            pltpu.VMEM(grad.shape, BF16), pltpu.VMEM(ig.shape, F32), dma((3,)), dma((3,)),
        ],
        compiler_params=pltpu.CompilerParams(vmem_limit_bytes=67043328),
    )(grad, ig, pen)
    return grad, ig, pen.reshape(())


def solution(mesh, dims=None):
    if dims is None:
        dims = (NX, NZ, NC, mesh.shape["rep"], CAP)
    both = ("expert", "rep")
    return jax.shard_map(
        functools.partial(body, dims),
        mesh=mesh,
        in_specs=(
            P(both, None), P(both, None),
            P("expert", None, None), P("expert", None, None),
            P(both, None), P(both, None),
        ),
        out_specs=(P("expert", "rep", None), P(both, None), P()),
        check_vma=False,
    )
```
